128 devices in a mesh: pw: 16 (over y_hi, x, core), ka: 8 (over z, y_lo).
Axes of the slice: x: 4, y: 4 (y_hi: 2, y_lo: 2; y = y_hi * 2 + y_lo), z: 4, core: 2. Of those that a mesh axis runs over, the one named last changes fastest.
Arguments:
- waves: bfloat16 [8, 2, 32768, 256], P('ka', None, 'pw'), may hold values from -0.125 to 0.125
- projectors: bfloat16 [8, 2, 32768, 2304], P('ka', None, 'pw'), may hold values from -0.125 to 0.125
- projector_order: int32 [2304], replicated, may hold values from 0 to 2303, each once
- shift_map: int32 [32768], P('pw'), may hold values from 0 to 32767, as said below
- charges: float32 [128, 18, 18], replicated, may hold values from -0.125 to 0.125
- atom_phase: float32 [128], replicated, may hold values from -3.140625 to 3.140625
Outputs:
- margins: float32 [8, 256, 2, 256], P('ka', 'pw')
The draws below stay inside these ranges and needn't reach their ends.
Inputs may be any that keep to these rules, and one draw needn't show every extreme that they name: `projector_order`: each projector slot once. `shift_map`: a permutation of the plane waves that maps every aligned block of 2048 plane waves onto itself.
All inputs are finite; a program needn't handle non-finite values.
Results may differ from the reference program's by a relative error of at most 0.0003.
Values may be sent and summed in bfloat16 or wider, within the bound.
A program may use at most 128 MiB of HBM per device.

```python
import jax
import jax.numpy as jnp
from jax import lax

NB = 256
PPA = 18
PW_DEV = 2048
KPTS = 8
NPW = 32768
ATOMS = 128
NPROJ = 2304


def draw_shift_map(key, part):
    blocks = NPW // PW_DEV
    keys = jax.random.split(key, blocks)
    perms = jax.vmap(lambda single: jax.random.permutation(single, PW_DEV))(keys)
    offsets = (jnp.arange(blocks, dtype=jnp.int32) * PW_DEV)[:, None]
    return (perms.astype(jnp.int32) + offsets).reshape(-1).astype(jnp.int32)


def level_of(rng, extent, shards, low, high):
    def one(position, parts):
        steps = jax.random.uniform(jax.random.fold_in(jax.random.fold_in(rng, 6), position), (parts,), jnp.float32, low / len(shards), high / len(shards))
        return jnp.repeat(jnp.exp(steps), extent[position] // parts).reshape((-1,) + (1,) * (len(extent) - position - 1))

    gain = one(*shards[0])
    for cut in shards[1:]:
        gain = gain * one(*cut)
    return gain


def gaussian(key, dims, width, reach, cuts=(), kind=jnp.bfloat16):
    factor_of = level_of(key, dims, cuts, -0.22, 0.18) if cuts else 1.0
    array = jax.random.normal(key, dims, jnp.float32) * width * factor_of
    return jnp.minimum(jnp.maximum(array, -reach), reach).astype(kind)


def setup_inputs(seed: int = 0) -> dict:
    seeds = jax.random.split(jax.random.key(seed), 7)
    waves = gaussian(seeds[0], (KPTS, 2, NPW, NB), (NPW // 16) ** -0.5, 0.125, ((0, 8), (2, 16)))
    projectors = gaussian(seeds[1], (KPTS, 2, NPW, NPROJ), (NPW // 16) ** -0.5, 0.125, ((0, 8), (2, 16)))
    projector_order = jax.random.permutation(seeds[2], NPROJ).astype(jnp.int32)
    shift_map = draw_shift_map(jax.random.fold_in(seeds[6], 71), 0)
    charges = gaussian(seeds[4], (ATOMS, PPA, PPA), NPROJ ** -0.5, 0.125, (), jnp.float32)
    atom_phase = jnp.clip(jax.random.uniform(seeds[5], (ATOMS,), jnp.float32, -3.140625, 3.140625), -3.140625, 3.140625)
    return {"waves": waves, "projectors": projectors, "projector_order": projector_order, "shift_map": shift_map, "charges": charges, "atom_phase": atom_phase}


def contract(left, right, precision=None):
    return lax.dot_general(left, right, (((0,), (0,)), ((), ())), precision=precision, preferred_element_type=jnp.float32)


def complex_cross(left, right, precision=None):
    real = contract(left[0], right[0], precision) + contract(left[1], right[1], precision)
    imag = contract(left[0], right[1], precision) - contract(left[1], right[0], precision)
    return jnp.stack([real, imag], axis=1)


def reference(waves, projectors, projector_order, shift_map, charges, atom_phase):
    inverse = jnp.argsort(projector_order).astype(jnp.int32)
    sym = 0.5 * (charges + jnp.transpose(charges, (0, 2, 1)))

    def project(pair):
        wave, beta = pair
        real = contract(beta[0], wave[0]) + contract(beta[1], wave[1])
        imag = contract(beta[0], wave[1]) - contract(beta[1], wave[0])
        return jnp.stack([real, imag])[:, inverse, :]

    proj = lax.map(project, (waves, projectors))
    last_wave = waves[0][:, shift_map.astype(jnp.int32), :]
    next_wave = jnp.concatenate([waves[1:], last_wave[None]], axis=0)
    repeated = jnp.repeat(atom_phase, PPA)
    cosine = jnp.cos(repeated)[:, None]
    sine = jnp.sin(repeated)[:, None]
    first = proj[0]
    rotated = jnp.stack([first[0] * cosine + first[1] * sine, first[1] * cosine - first[0] * sine])
    next_proj = jnp.concatenate([proj[1:], rotated[None]], axis=0)

    def margin(items):
        wave, nwave, pk, pn = items
        plane = complex_cross(wave, nwave)
        split = pn.reshape(2, ATOMS, PPA, NB)
        weighted = jnp.einsum("apq,raqj->rapj", sym, split, precision=lax.Precision.HIGHEST).reshape(2, NPROJ, NB)
        aug = complex_cross(pk, weighted, lax.Precision.HIGHEST)
        return plane + aug

    return lax.map(margin, (waves, next_wave, proj, next_proj))
```

```python
import jax
import jax.numpy as jnp
from jax import lax
from jax.experimental import pallas as pl
from jax.experimental.pallas import tpu as pltpu
from jax.sharding import PartitionSpec as P

MESH = pl.DeviceIdType.MESH
HIGH = lax.Precision.HIGHEST
F32 = jnp.float32
BF16 = jnp.bfloat16

NPW = 2048
NB = 256
PPA = 18
NPROJ = 2304
COLS = 256
STEPS = NPROJ // COLS
PARTS = 2
SLOTS = 72
ROWS = 4 * SLOTS
WCH = 8
WROWS = NPW // WCH


def dot(a, b, dims=((1,), (0,)), precision=None):
    return lax.dot_general(a, b, (dims, ((), ())), precision=precision, preferred_element_type=F32)


def iota(shape, dim):
    return lax.broadcasted_iota(jnp.int32, shape, dim)


def kernel(
    order_ref, shift_ref, phase_ref, charges_ref, waves_ref, proj_ref, out_ref,
    wv, lt, beta, pu, ps, crecv, far, near, ydst, nxt, wsend, wnext,
    colb, invv, invs, chv, sym, plane, stage, oc, ocore, orecv, onehot,
    load_sem, beta_sem, misc_sem, core_s, core_r, x_s, far_r, near_r, y_s, y_r, n_s, n_r,
    w_s, w_r, oc_s, oc_r, o_s, o_r,
):
    me = lax.axis_index("pw")
    ka = lax.axis_index("ka")
    core = lax.rem(me, 2)
    j = me // 2
    x = lax.rem(j, 4)
    h = j // 4
    oh = 1 - h
    right = lax.rem(x + 1, 4)
    left = lax.rem(x + 3, 4)
    across = lax.rem(x + 2, 4)
    before = lax.rem(ka + 7, 8)
    after = lax.rem(ka + 1, 8)
    first = ka == 0
    last = ka == 7

    def pw_of(hh, xx, cc):
        return (hh * 4 + xx) * 2 + cc

    def send(src, dst, s, r, pw, k):
        return pltpu.make_async_remote_copy(src_ref=src, dst_ref=dst, send_sem=s, recv_sem=r, device_id=(pw, k), device_id_type=MESH)

    load = pltpu.make_async_copy(waves_ref.at[0], wv, load_sem)
    load.start()

    def beta_copy(i):
        src = proj_ref.at[0, :, :, pl.ds(pl.multiple_of(i * COLS, COLS), COLS)]
        return pltpu.make_async_copy(src, beta.at[i], beta_sem.at[i])

    for i in range(STEPS):
        beta_copy(i).start()
    ch_copy = pltpu.make_async_copy(charges_ref.at[pl.ds(8 * me, 8)], chv, misc_sem.at[0])
    ch_copy.start()

    barrier = pltpu.get_barrier_semaphore()
    for d in range(1, 16):
        pl.semaphore_signal(barrier, inc=1, device_id=(lax.rem(me + d, 16), ka), device_id_type=MESH)
    for k in (before, after):
        pl.semaphore_signal(barrier, inc=1, device_id=(me, k), device_id_type=MESH)
    pl.semaphore_wait(barrier, 17)

    def w_copy(c, src):
        return send(src, wnext.at[:, pl.ds(pl.multiple_of(c * WROWS, WROWS), WROWS), :], w_s.at[c], w_r.at[c], me, before)

    def rows_of(ref, c):
        return ref.at[:, pl.ds(pl.multiple_of(c * WROWS, WROWS), WROWS), :]

    @pl.when(jnp.logical_not(first))
    def _():
        for c in range(WCH):
            w_copy(c, waves_ref.at[0, :, pl.ds(c * WROWS, WROWS), :]).start()

    load.wait()

    @pl.when(first)
    def _():
        def piece(c, _):
            for half in range(WROWS // 128):
                row = shift_ref[pl.ds(c * (WROWS // 128) + half, 1), :] - me * NPW
                want = jnp.broadcast_to(row.astype(F32), (128, 128)).T
                for t in range(NPW // 128):
                    have = (iota((128, 128), 1) + 128 * t).astype(F32)
                    onehot[:, 128 * t : 128 * (t + 1)] = jnp.where(want == have, 1.0, 0.0).astype(BF16)
                at = pl.ds(pl.multiple_of(c * WROWS + half * 128, 128), 128)
                for r in range(2):
                    wsend[r, at, :] = dot(onehot[...], wv[r]).astype(BF16)
            w_copy(c, rows_of(wsend, c)).start()
            return 0

        lax.fori_loop(0, WCH, piece, 0)

    for r in range(NPROJ // 128):
        row = order_ref[pl.ds(r, 1), :].astype(F32)
        colb[pl.ds(128 * r, 128), :] = jnp.broadcast_to(row, (128, 128)).T

    def invert(b, _):
        slot = (iota((NPROJ, 128), 1) + 128 * b).astype(F32)
        hit = jnp.where(colb[...] == slot, (iota((NPROJ, 128), 0) * 4).astype(F32), 0.0)
        found = jnp.sum(hit, axis=0, keepdims=True).astype(jnp.int32)
        invv[pl.ds(b, 1), :] = jnp.clip(found, 0, 4 * (NPROJ - 1))
        return 0

    lax.fori_loop(0, NPROJ // 128, invert, 0)
    inv_copy = pltpu.make_async_copy(invv, invs, misc_sem.at[1])
    inv_copy.start()

    for c in range(8):
        g = slice(256 * c, 256 * (c + 1))
        gi = slice(NPW + 256 * c, NPW + 256 * (c + 1))
        re = wv[0, g, :].T
        im = wv[1, g, :].T
        lt[0:NB, g] = re
        lt[0:NB, gi] = im
        lt[NB:, g] = im
        lt[NB:, gi] = -re

    def project(i, _):
        beta_copy(i).wait()
        acc = dot(lt[...], beta[i].reshape(2 * NPW, COLS))
        for q in range(4):
            pu[pl.ds(pl.multiple_of(4 * COLS * i, 8) + q, COLS, stride=4), :] = acc[128 * q : 128 * (q + 1), :].T
        return 0

    lax.fori_loop(0, STEPS, project, 0)
    inv_copy.wait()

    def gather(c, cr):
        def block(b, _):
            s0 = (2 * b + cr) * 2 * SLOTS + c * SLOTS

            def body(i, _):
                for u in range(8):
                    n = i * 8 + u
                    s = s0 + n
                    r = invs[s >> 7, s & 127]
                    ps[c, cr, b, pl.ds(pl.multiple_of(4 * n, 4), 4), :] = pu[pl.ds(r, 4), :]
                return 0

            return lax.fori_loop(0, SLOTS // 8, body, 0)

        lax.fori_loop(0, 8, block, 0)

    pw_core = pw_of(h, x, 1 - core)
    pw_right = pw_of(h, right, core)
    pw_left = pw_of(h, left, core)
    pw_y = pw_of(oh, x, core)

    def core_copy(c):
        return send(ps.at[c, 1 - core], crecv.at[c], core_s.at[c], core_r.at[c], pw_core, ka)

    for c in range(PARTS):
        gather(c, 1 - core)
        core_copy(c).start()
        gather(c, core)

    def block_of(hh, xx):
        return hh * 4 + xx

    def mine(c, b):
        return ps.at[c, core, b]

    def far_copy(c, d):
        return send(mine(c, block_of(d, across)), far.at[c, d], x_s.at[c, d], far_r.at[c, d], (pw_right, pw_left)[d], ka)

    def near_copy(c, d, hh):
        return send(
            mine(c, block_of(hh, (right, left)[d])), near.at[c, d, hh], x_s.at[c, 2 + 2 * d + hh], near_r.at[c, d, hh],
            (pw_right, pw_left)[d], ka,
        )

    def add_core(c, b):
        ps[c, core, b] += crecv[c, b]

    for c in range(PARTS):
        core_copy(c).wait_recv()
        for d in range(2):
            add_core(c, block_of(d, across))
            far_copy(c, d).start()
        for d in range(2):
            add_core(c, block_of(1 - d, (right, left)[d]))
            near_copy(c, d, 1 - d).start()
        for d in range(2):
            add_core(c, block_of(d, (right, left)[d]))
        for hh in range(2):
            add_core(c, block_of(hh, x))
    for c in range(PARTS):
        for d in range(2):
            far_copy(c, d).wait_recv()
            ps[c, core, block_of(d, (right, left)[d])] += far[c, d]
            near_copy(c, d, d).start()

    def y_copy(c):
        return send(mine(c, block_of(oh, x)), ydst.at[c], y_s.at[c], y_r.at[c], pw_y, ka)

    def n_copy(c):
        return send(mine(c, block_of(h, x)), nxt.at[c], n_s.at[c], n_r.at[c], me, before)

    for c in range(PARTS):
        for d in range(2):
            for hh in range(2):
                near_copy(c, d, hh).wait_recv()
        ps[c, core, block_of(oh, x)] += near[c, 0, oh] + near[c, 1, oh]
        y_copy(c).start()
        ps[c, core, block_of(h, x)] += near[c, 0, h] + near[c, 1, h]
    for c in range(PARTS):
        y_copy(c).wait_recv()
        ps[c, core, block_of(h, x)] += ydst[c]
        n_copy(c).start()

    ch_copy.wait()
    slot_r = iota((SLOTS, PPA), 0)
    chan_c = iota((SLOTS, PPA), 1)
    atom_row = ((iota((SLOTS, SLOTS), 0).astype(F32) + 0.5) * (1.0 / PPA)).astype(jnp.int32)
    atom_col = ((iota((SLOTS, SLOTS), 1).astype(F32) + 0.5) * (1.0 / PPA)).astype(jnp.int32)
    same = atom_row == atom_col
    spread = jnp.zeros((PPA, SLOTS), F32)
    for a in range(SLOTS // PPA):
        spread += jnp.where(iota((PPA, SLOTS), 1) == iota((PPA, SLOTS), 0) + PPA * a, 1.0, 0.0)
    for c in range(PARTS):
        flat = jnp.zeros((SLOTS, PPA), F32)
        for a in range(SLOTS // PPA):
            pick = jnp.where(slot_r == chan_c + PPA * a, 1.0, 0.0).astype(F32)
            charge = chv[c * (SLOTS // PPA) + a]
            flat += dot(pick, charge, precision=HIGH) + dot(pick, charge, ((1,), (1,)), HIGH)
        sym[c] = jnp.where(same, dot(0.5 * flat, spread, precision=HIGH), 0.0)

    def wide(ref, lo):
        return jnp.concatenate([ref[pl.ds(lo, SLOTS, stride=4), :], ref[pl.ds(lo + 1, SLOTS, stride=4), :]], axis=1)

    colb[0:128, :] = jnp.broadcast_to(phase_ref[...], (128, 128)).T
    own = colb[pl.ds(pl.multiple_of(8 * me, 8), 8), :]
    cosine = jnp.cos(own)
    sine = jnp.sin(own)

    total = jnp.zeros((NB, 2 * NB), F32)
    for c in range(PARTS):
        n_copy(c).wait_recv()
        nr = wide(nxt.at[c], 0)
        ni = wide(nxt.at[c], 2)
        repeat = jnp.where(((iota((SLOTS, 8), 0).astype(F32) + 0.5) * (1.0 / PPA)).astype(jnp.int32) + c * (SLOTS // PPA) == iota((SLOTS, 8), 1), 1.0, 0.0)
        cc = dot(repeat, cosine, precision=HIGH)
        sc = dot(repeat, sine, precision=HIGH)
        cc = jnp.where(last, jnp.concatenate([cc, cc], axis=1), 1.0)
        sc = jnp.where(last, jnp.concatenate([sc, sc], axis=1), 0.0)
        turned = jnp.concatenate([nr * cc + ni * sc, ni * cc - nr * sc], axis=1)
        weighted = dot(sym[c], turned, precision=HIGH)
        wr = weighted[:, :NB]
        wi = weighted[:, NB:]
        pk = ps.at[c, core, block_of(h, x)]
        pr = wide(pk, 0)
        pi = wide(pk, 2)
        total += dot(pr, jnp.concatenate([wr, wi], axis=1), ((0,), (0,)), HIGH)
        total += dot(pi, jnp.concatenate([wi, -wr], axis=1), ((0,), (0,)), HIGH)
    stage[...] = total

    plane[...] = jnp.zeros_like(plane)

    def product(i, _):
        w_copy(2 * i, rows_of(wsend, 2 * i)).wait_recv()
        w_copy(2 * i + 1, rows_of(wsend, 2 * i + 1)).wait_recv()
        g = pl.ds(pl.multiple_of(2 * WROWS * i, 128), 2 * WROWS)
        gi = pl.ds(pl.multiple_of(NPW + 2 * WROWS * i, 128), 2 * WROWS)
        plane[...] += dot(lt[:, g], wnext[0, g, :]) + dot(lt[:, gi], wnext[1, g, :])
        return 0

    lax.fori_loop(0, WCH // 2, product, 0)

    for p in range(16):
        rows = slice(16 * p, 16 * (p + 1))
        oc[p % 2, p // 2, 0] = stage[rows, :NB] + plane[rows, :]
        oc[p % 2, p // 2, 1] = stage[rows, NB:] - plane[NB + 16 * p : NB + 16 * (p + 1), :]
    o_core = send(oc.at[1 - core], ocore, oc_s, oc_r, pw_core, ka)
    o_core.start()
    o_core.wait_recv()
    for b in range(8):
        oc[core, b] += ocore[b]

    def o_copy(d):
        to = lax.rem(j + d, 8)
        return send(oc.at[core, to], orecv.at[d], o_s.at[d], o_r.at[d], 2 * to + core, ka)

    for d in range(1, 8):
        o_copy(d).start()
    result = oc[core, j]
    for d in range(1, 8):
        o_copy(d).wait_recv()
        result += orecv[d]
    out_ref[0, :, 0, :] = result[0]
    out_ref[0, :, 1, :] = result[1]

    o_core.wait_send()
    for d in range(1, 8):
        o_copy(d).wait_send()
    for c in range(WCH):
        w_copy(c, rows_of(wsend, c)).wait_send()
    for c in range(PARTS):
        core_copy(c).wait_send()
        y_copy(c).wait_send()
        n_copy(c).wait_send()
        for d in range(2):
            far_copy(c, d).wait_send()
            for hh in range(2):
                near_copy(c, d, hh).wait_send()


def local(waves, projectors, projector_order, shift_map, charges, atom_phase):
    vmem = pl.BlockSpec(memory_space=pltpu.VMEM)
    hbm = pl.BlockSpec(memory_space=pl.ANY)
    dma = pltpu.SemaphoreType.DMA
    return pl.pallas_call(
        kernel,
        out_shape=jax.ShapeDtypeStruct((1, 16, 2, NB), F32),
        in_specs=[vmem, vmem, vmem, hbm, hbm, hbm],
        out_specs=vmem,
        scratch_shapes=[
            pltpu.VMEM((2, NPW, NB), BF16),
            pltpu.VMEM((2 * NB, 2 * NPW), BF16),
            pltpu.VMEM((STEPS, 2, NPW, COLS), BF16),
            pltpu.VMEM((4 * NPROJ, 128), F32),
            pltpu.VMEM((PARTS, 2, 8, ROWS, 128), F32),
            pltpu.VMEM((PARTS, 8, ROWS, 128), F32),
            pltpu.VMEM((PARTS, 2, ROWS, 128), F32),
            pltpu.VMEM((PARTS, 2, 2, ROWS, 128), F32),
            pltpu.VMEM((PARTS, ROWS, 128), F32),
            pltpu.VMEM((PARTS, ROWS, 128), F32),
            pltpu.VMEM((2, NPW, NB), BF16),
            pltpu.VMEM((2, NPW, NB), BF16),
            pltpu.VMEM((NPROJ, 128), F32),
            pltpu.VMEM((NPROJ // 128, 128), jnp.int32),
            pltpu.SMEM((NPROJ // 128, 128), jnp.int32),
            pltpu.VMEM((8, PPA, PPA), F32),
            pltpu.VMEM((PARTS, SLOTS, SLOTS), F32),
            pltpu.VMEM((2 * NB, NB), F32),
            pltpu.VMEM((NB, 2 * NB), F32),
            pltpu.VMEM((2, 8, 2, 16, NB), F32),
            pltpu.VMEM((8, 2, 16, NB), F32),
            pltpu.VMEM((8, 2, 16, NB), F32),
            pltpu.VMEM((128, NPW), BF16),
            dma, dma((STEPS,)), dma((2,)),
            dma((PARTS,)), dma((PARTS,)),
            dma((PARTS, 6)), dma((PARTS, 2)), dma((PARTS, 2, 2)),
            dma((PARTS,)), dma((PARTS,)), dma((PARTS,)), dma((PARTS,)),
            dma((WCH,)), dma((WCH,)),
            dma, dma, dma((8,)), dma((8,)),
        ],
        compiler_params=pltpu.CompilerParams(collective_id=0, has_side_effects=True, vmem_limit_bytes=64 * 1024 * 1024 - 65536),
    )(
        projector_order.reshape(NPROJ // 128, 128),
        shift_map.reshape(NPW // 128, 128),
        atom_phase.reshape(1, 128),
        charges,
        waves,
        projectors,
    )


def solution(mesh):
    in_specs = (P("ka", None, "pw", None), P("ka", None, "pw", None), P(), P("pw"), P(), P())
    out_specs = P("ka", "pw", None, None)
    return jax.shard_map(local, mesh=mesh, in_specs=in_specs, out_specs=out_specs, check_vma=False)
```

```python
import jax
import jax.numpy as jnp
from jax import lax
from jax.experimental import pallas as pl
from jax.experimental.pallas import tpu as pltpu
from jax.sharding import PartitionSpec as P

MESH = pl.DeviceIdType.MESH
HIGH = lax.Precision.HIGHEST
F32 = jnp.float32
BF16 = jnp.bfloat16

NPW = 2048
NB = 256
PPA = 18
NPROJ = 2304
COLS = 256
STEPS = NPROJ // COLS
PARTS = 2
HALF = NB // PARTS
SLOTS = 144
SUB = 1
ROWS = 2 * SLOTS
OWN = NPW // 2
WCH = 8
WROWS = OWN // WCH
XCH = 4
EXTRA = OWN // 2
SPLIT = 6


def dot(a, b, dims=((1,), (0,)), precision=None):
    return lax.dot_general(a, b, (dims, ((), ())), precision=precision, preferred_element_type=F32)


def iota(shape, dim):
    return lax.broadcasted_iota(jnp.int32, shape, dim)


def kernel(
    order_ref, shift_ref, phase_ref, charges_ref, waves_ref, proj_ref, out_ref,
    wv, lt, beta, pu, ps, crecv, far, near, ydst, nxt, pk, xw, yw, ew, es, lp,
    colb, acc, invv, invs, sym, turn, bra, ket, plane, stage, oc, ocore, orecv, onehot,
    load_sem, beta_sem, inv_sem, core_s, core_r, x_s, far_r, near_r, y_s, y_r, n_s, n_r,
    w_s, w_r, f_s, f_r, e_s, e_r, oc_s, oc_r, o_s, o_r,
):
    me = lax.axis_index("pw")
    ka = lax.axis_index("ka")
    core = lax.rem(me, 2)
    j = me // 2
    x = lax.rem(j, 4)
    h = j // 4
    oh = 1 - h
    right = lax.rem(x + 1, 4)
    left = lax.rem(x + 3, 4)
    across = lax.rem(x + 2, 4)
    before = lax.rem(ka + 7, 8)
    after = lax.rem(ka + 1, 8)
    first = ka == 0
    last = ka == 7
    odd = lax.rem(ka, 2)
    partner = ka + 1 - 2 * odd
    beyond = lax.rem(ka + 2 + 4 * odd, 8)
    sent = OWN * (1 - odd)
    kept = OWN * odd

    def pw_of(hh, xx, cc):
        return (hh * 4 + xx) * 2 + cc

    def send(src, dst, s, r, pw, k):
        return pltpu.make_async_remote_copy(src_ref=src, dst_ref=dst, send_sem=s, recv_sem=r, device_id=(pw, k), device_id_type=MESH)

    load = pltpu.make_async_copy(waves_ref.at[0], wv, load_sem)
    load.start()

    def beta_copy(i):
        src = proj_ref.at[0, :, :, pl.ds(pl.multiple_of(i * COLS, COLS), COLS)]
        return pltpu.make_async_copy(src, beta.at[i], beta_sem.at[i])

    for i in range(2):
        beta_copy(i).start()

    pw_y = pw_of(oh, x, core)
    barrier = pltpu.get_barrier_semaphore()
    peers = [(lax.rem(me + d, 16), ka) for d in range(1, 16)]
    peers += [(me, lax.rem(ka + d, 8)) for d in (2, 6)]
    peers += [(2 * lax.rem(j + d, 8) + core, k) for d in range(8) for k in (before, after)]
    for peer in peers:
        pl.semaphore_signal(barrier, inc=1, device_id=peer, device_id_type=MESH)

    order = jnp.concatenate([order_ref[pl.ds(r, 1), :] for r in range(NPROJ // 128)], axis=1)
    column = iota((SLOTS, NPROJ), 1)
    match_hi = (order >> 4) == iota((SLOTS, NPROJ), 0)
    match_lo = jnp.where((order & 15) == iota((16, NPROJ), 0), 1.0, 0.0).astype(BF16)
    digit_hi = jnp.where(match_hi, (column >> 7).astype(F32), 0.0).astype(BF16)
    digit_lo = jnp.where(match_hi, (column & 127).astype(F32), 0.0).astype(BF16)
    found = dot(digit_hi, match_lo, ((1,), (1,))) * 128.0 + dot(digit_lo, match_lo, ((1,), (1,)))
    invv[...] = jnp.clip(2 * found.astype(jnp.int32), 0, 2 * (NPROJ - 1))
    inv_copy = pltpu.make_async_copy(invv, invs, inv_sem)
    inv_copy.start()

    load.wait()
    for i in range(2, STEPS):
        beta_copy(i).start()

    for c in range(8):
        g = slice(256 * c, 256 * (c + 1))
        gi = slice(NPW + 256 * c, NPW + 256 * (c + 1))
        re = wv[0, g, :].T
        im = wv[1, g, :].T
        for p in range(PARTS):
            bands = slice(HALF * p, HALF * (p + 1))
            lt[NB * p : NB * p + HALF, g] = re[bands]
            lt[NB * p : NB * p + HALF, gi] = im[bands]
            lt[NB * p + HALF : NB * (p + 1), g] = im[bands]
            lt[NB * p + HALF : NB * (p + 1), gi] = -re[bands]

    pl.semaphore_wait(barrier, len(peers))

    def piece(ref, c):
        return ref.at[:, pl.ds(c * WROWS, WROWS), :]

    def w_copy(c):
        src = waves_ref.at[0, :, pl.ds(pl.multiple_of(sent + c * WROWS, WROWS), WROWS), :]
        return send(src, piece(xw, c), w_s.at[c], w_r.at[c], me, partner)

    def f_copy(c):
        return send(piece(xw, c), piece(yw, c), f_s.at[c], f_r.at[c], me, beyond)

    def to_last(c):
        return send(piece(es, c), piece(yw, c), e_s.at[c], f_r.at[c], me, before)

    def to_first(c):
        src = waves_ref.at[0, :, pl.ds(OWN + EXTRA + c * WROWS, WROWS), :]
        return send(src, piece(ew, c), e_s.at[c], e_r.at[c], me, after)

    for c in range(WCH):
        w_copy(c).start()

    @pl.when(last)
    def _():
        for c in range(XCH):
            to_first(c).start()

    def forward(lo, hi):
        for c in range(lo, hi):
            w_copy(c).wait_recv()

        @pl.when(ka != 1)
        def _():
            for c in range(lo, hi):
                f_copy(c).start()

    def choose(group):
        row = shift_ref[pl.ds(group, 1), :] - me * NPW
        want = jnp.broadcast_to(row.astype(F32), (128, 128)).T
        for t in range(NPW // 128):
            have = (iota((128, 128), 1) + 128 * t).astype(F32)
            onehot[:, 128 * t : 128 * (t + 1)] = jnp.where(want == have, 1.0, 0.0).astype(BF16)

    def extra_first():
        @pl.when(first)
        def _():
            def body(t, _):
                choose(OWN // 128 + t)
                for r in range(2):
                    es[r, pl.ds(pl.multiple_of(128 * t, 128), 128), :] = dot(onehot[...], wv[r]).astype(BF16)
                return 0

            lax.fori_loop(0, EXTRA // 128, body, 0)
            for c in range(XCH):
                to_last(c).start()

    def permute_first():
        @pl.when(first)
        def _():
            def body(t, _):
                choose(t + jnp.where(t >= OWN // 128, EXTRA // 128, 0))
                got = dot(lt[:, 0:NPW], onehot[...], ((1,), (1,))).astype(BF16)
                at = pl.multiple_of(128 * t, 128)
                lp[:, pl.ds(at, 128)] = got
                for p in range(PARTS):
                    lo = NB * p
                    lp[lo : lo + HALF, pl.ds(OWN + EXTRA + at, 128)] = got[lo + HALF : lo + NB]
                    lp[lo + HALF : lo + NB, pl.ds(OWN + EXTRA + at, 128)] = -got[lo : lo + HALF]
                return 0

            lax.fori_loop(0, (OWN + EXTRA) // 128, body, 0)

    def put(c, i):
        for q in range(2):
            pu[c, pl.ds(pl.multiple_of(2 * COLS * i, 8) + q, COLS, stride=2), :] = acc[HALF * q : HALF * (q + 1), :].T

    def project(c, lo, hi):
        def body(i, _):
            if c == 0:
                beta_copy(i).wait()
            put(c, jnp.maximum(i - 1, lo))
            acc[...] = dot(lt[NB * c : NB * (c + 1), :], beta[i].reshape(2 * NPW, COLS))
            return 0

        lax.fori_loop(lo, hi, body, 0)
        put(c, hi - 1)

    def gather(c, cr):
        def block(b, _):
            dst = ps.at[c, cr, b]

            def body(i, _):
                rows = [invs[9 * (2 * b + cr) + i, u] for u in range(16)]
                got = [pu[c, pl.ds(r, 2), :] for r in rows]
                for u in range(16):
                    dst[pl.ds(pl.multiple_of(32 * i, 32) + 2 * u, 2), :] = got[u]
                return 0

            return lax.fori_loop(0, SLOTS // 16, body, 0)

        lax.fori_loop(0, 8, block, 0)

    pw_core = pw_of(h, x, 1 - core)
    pw_right = pw_of(h, right, core)
    pw_left = pw_of(h, left, core)
    def core_copy(c):
        return send(ps.at[c, 1 - core], crecv.at[c], core_s.at[c], core_r.at[c], pw_core, ka)

    def spread_out(c):
        gather(c, 1 - core)
        core_copy(c).start()
        gather(c, core)

    def block_of(hh, xx):
        return hh * 4 + xx

    def sub(ref, e):
        return ref.at[pl.ds(e * (ROWS // SUB), ROWS // SUB), :]

    def mine(c, e, b):
        return sub(ps.at[c, core, b], e)

    def far_copy(c, e, d):
        return send(
            mine(c, e, block_of(d, across)), sub(far.at[c, d], e), x_s.at[c, e, d], far_r.at[c, e, d], (pw_right, pw_left)[d], ka
        )

    def near_copy(c, e, d, hh):
        return send(
            mine(c, e, block_of(hh, (right, left)[d])), sub(near.at[c, d, hh], e), x_s.at[c, e, 2 + 2 * d + hh],
            near_r.at[c, e, d, hh], (pw_right, pw_left)[d], ka,
        )

    def add_core(c, b):
        ps[c, core, b] += crecv[c, b]

    def ring_start(c):
        core_copy(c).wait_recv()
        for d in range(2):
            add_core(c, block_of(d, across))
            for e in range(SUB):
                far_copy(c, e, d).start()
        for d in range(2):
            add_core(c, block_of(1 - d, (right, left)[d]))
            for e in range(SUB):
                near_copy(c, e, d, 1 - d).start()
        for d in range(2):
            add_core(c, block_of(d, (right, left)[d]))
        for hh in range(2):
            add_core(c, block_of(hh, x))

    def add(c, e, b, ref):
        at = pl.ds(e * (ROWS // SUB), ROWS // SUB)
        total = ps[c, core, b, at, :]
        for one in ref:
            total += one[at, :]
        ps[c, core, b, at, :] = total

    def ring_rest(c):
        for e in range(SUB):
            for d in range(2):
                far_copy(c, e, d).wait_recv()
                add(c, e, block_of(d, (right, left)[d]), [far.at[c, d]])
                near_copy(c, e, d, d).start()

    def y_copy(c, e):
        return send(mine(c, e, block_of(oh, x)), sub(ydst.at[c], e), y_s.at[c, e], y_r.at[c, e], pw_y, ka)

    def n_copy(c, e, d):
        return send(
            mine(c, e, block_of((h, oh)[d], x)), sub(nxt.at[c, d], e), n_s.at[c, e, d], n_r.at[c, e, d], (me, pw_y)[d], before
        )

    def ring_end(c):
        for e in range(SUB):
            for d in range(2):
                for hh in range(2):
                    near_copy(c, e, d, hh).wait_recv()
            add(c, e, block_of(oh, x), [near.at[c, 0, oh], near.at[c, 1, oh]])
            y_copy(c, e).start()
            n_copy(c, e, 1).start()
            add(c, e, block_of(h, x), [near.at[c, 0, h], near.at[c, 1, h]])
            n_copy(c, e, 0).start()

    acc[...] = jnp.zeros_like(acc)
    project(0, 0, STEPS)
    inv_copy.wait()
    spread_out(0)
    forward(0, 2)
    project(1, 0, SPLIT)
    ring_start(0)
    project(1, SPLIT, STEPS)
    forward(2, 4)
    spread_out(1)
    extra_first()
    ring_rest(0)
    forward(4, 6)
    ring_start(1)

    atom_row = ((iota((SLOTS, SLOTS), 0).astype(F32) + 0.5) * (1.0 / PPA)).astype(jnp.int32)
    atom_col = ((iota((SLOTS, SLOTS), 1).astype(F32) + 0.5) * (1.0 / PPA)).astype(jnp.int32)
    spread = jnp.zeros((PPA, SLOTS), F32)
    for a in range(SLOTS // PPA):
        spread += jnp.where(iota((PPA, SLOTS), 1) == iota((PPA, SLOTS), 0) + PPA * a, 1.0, 0.0)
    slot = iota((SLOTS, 128), 0)
    atom = iota((SLOTS, 128), 1) - 8 * me
    flat = jnp.zeros((SLOTS, PPA), F32)
    for p in range(PPA):
        pick = jnp.where(slot == PPA * atom + p, 1.0, 0.0)
        flat += dot(pick, 0.5 * (charges_ref[p] + charges_ref[:, p, :]), ((1,), (1,)), HIGH)
    sym[...] = jnp.where(atom_row == atom_col, dot(flat, spread, precision=HIGH), 0.0)

    colb[...] = jnp.broadcast_to(phase_ref[...], (128, 128)).T
    own = colb[pl.ds(pl.multiple_of(8 * me, 8), 8), :]
    repeat = jnp.where(((iota((SLOTS, 8), 0).astype(F32) + 0.5) * (1.0 / PPA)).astype(jnp.int32) == iota((SLOTS, 8), 1), 1.0, 0.0)
    turn[0] = jnp.where(last, dot(repeat, jnp.cos(own), precision=HIGH), 1.0)
    turn[1] = jnp.where(last, dot(repeat, jnp.sin(own), precision=HIGH), 0.0)

    forward(6, 8)
    permute_first()
    ring_end(0)

    def product(left, at, width, parts):
        total = None
        for r in range(2):
            for ref, lo, n in parts:
                term = dot(left[:, pl.ds(pl.multiple_of(at + r * width + lo, 128), n)], ref[r, 0:n, :])
                total = term if total is None else total + term
        return total

    def f_wait(lo, hi):
        for c in range(lo, hi):
            f_copy(c).wait_recv()

    plane[odd] = product(lt, kept, NPW, [(xw, 0, OWN)])
    ring_rest(1)
    ring_end(1)

    @pl.when(jnp.logical_not(first | last))
    def _():
        f_wait(0, WCH)
        plane[1 - odd] = product(lt, kept, NPW, [(yw, 0, OWN)])

    @pl.when(last)
    def _():
        f_wait(0, XCH)
        plane[1 - odd] = product(lt, kept, NPW, [(yw, 0, EXTRA)])

    @pl.when(first)
    def _():
        f_wait(0, WCH)
        for c in range(XCH):
            to_first(c).wait_recv()
        plane[1 - odd] = product(lp, 0, OWN + EXTRA, [(yw, 0, OWN), (ew, OWN, EXTRA)])

    for c in range(PARTS):
        for r in range(2):
            lo = NB * c + HALF * r
            turned = plane[1, lo : lo + HALF, :].T
            for p in range(16):
                oc[1, p % 2, p // 2, r, :, HALF * c : HALF * (c + 1)] = turned[16 * p : 16 * (p + 1)]

    def o_core(t):
        return send(oc.at[t, 1 - core], ocore.at[t], oc_s.at[t], oc_r.at[t], pw_core, ka)

    def o_copy(t, d):
        to = lax.rem(j + d, 8)
        return send(oc.at[t, core, to], orecv.at[t, d], o_s.at[t, d], o_r.at[t, d], 2 * to + core, (ka, before)[t])

    def o_start(t):
        o_core(t).wait_recv()
        for b in range(8):
            oc[t, core, b] += ocore[t, b]
        for d in range(1 - t, 8):
            o_copy(t, d).start()

    o_core(1).start()

    def rows(ref, q):
        return ref[pl.ds(q, SLOTS, stride=2), :]

    def weigh(c):
        for e in range(SUB):
            for d in range(2):
                n_copy(c, e, d).wait_recv()
        nxt[c, 0] += nxt[c, 1]
        nr = rows(nxt.at[c, 0], 0)
        ni = rows(nxt.at[c, 0], 1)
        both = jnp.concatenate([nr * turn[0] + ni * turn[1], ni * turn[0] - nr * turn[1]], axis=1)
        weighted = dot(sym[...], both, precision=HIGH)
        wr = weighted[:, :HALF]
        wi = weighted[:, HALF:]
        ket[0:SLOTS, NB * c : NB * c + HALF] = wr
        ket[0:SLOTS, NB * c + HALF : NB * (c + 1)] = wi
        ket[SLOTS:, NB * c : NB * c + HALF] = wi
        ket[SLOTS:, NB * c + HALF : NB * (c + 1)] = -wr

    def hold(c):
        for e in range(SUB):
            y_copy(c, e).wait_recv()
        pk[c] = ps[c, core, block_of(h, x)] + ydst[c]
        for q in range(2):
            bra[HALF * c : HALF * (c + 1), SLOTS * q : SLOTS * (q + 1)] = rows(pk.at[c], q).T

    hold(0)
    weigh(0)
    o_start(1)
    hold(1)
    weigh(1)
    stage[...] = dot(bra[...], ket[...], precision=HIGH)

    for p in range(16):
        at = slice(16 * p, 16 * (p + 1))
        lo = NB * (p // 8) + 16 * (p % 8)
        for c in range(PARTS):
            bands = slice(HALF * c, HALF * (c + 1))
            oc[0, p % 2, p // 2, 0, :, bands] = stage[at, NB * c : NB * c + HALF] + plane[0, lo : lo + 16, bands]
            oc[0, p % 2, p // 2, 1, :, bands] = stage[at, NB * c + HALF : NB * (c + 1)] - plane[0, lo + HALF : lo + HALF + 16, bands]
    o_core(0).start()

    o_start(0)
    result = oc[0, core, j]
    for t in (1, 0):
        for d in range(1 - t, 8):
            o_copy(t, d).wait_recv()
            result += orecv[t, d]
    for r in range(2):
        for p in range(PARTS):
            out_ref[pl.ds(2 * p + r, 16, stride=4), :] = result[r][:, HALF * p : HALF * (p + 1)]

    for t in range(2):
        o_core(t).wait_send()
        for d in range(1 - t, 8):
            o_copy(t, d).wait_send()
    for c in range(WCH):
        w_copy(c).wait_send()

    @pl.when(ka != 1)
    def _():
        for c in range(WCH):
            f_copy(c).wait_send()

    @pl.when(first)
    def _():
        for c in range(XCH):
            to_last(c).wait_send()

    @pl.when(last)
    def _():
        for c in range(XCH):
            to_first(c).wait_send()

    for c in range(PARTS):
        core_copy(c).wait_send()
        for e in range(SUB):
            y_copy(c, e).wait_send()
            for d in range(2):
                n_copy(c, e, d).wait_send()
                far_copy(c, e, d).wait_send()
                for hh in range(2):
                    near_copy(c, e, d, hh).wait_send()


def local(waves, projectors, projector_order, shift_map, charges, atom_phase):
    vmem = pl.BlockSpec(memory_space=pltpu.VMEM)
    hbm = pl.BlockSpec(memory_space=pl.ANY)
    dma = pltpu.SemaphoreType.DMA
    rows = pl.pallas_call(
        kernel,
        out_shape=jax.ShapeDtypeStruct((64, HALF), F32),
        in_specs=[vmem, vmem, vmem, vmem, hbm, hbm],
        out_specs=vmem,
        scratch_shapes=[
            pltpu.VMEM((2, NPW, NB), BF16),
            pltpu.VMEM((2 * NB, 2 * NPW), BF16),
            pltpu.VMEM((STEPS, 2, NPW, COLS), BF16),
            pltpu.VMEM((PARTS, 2 * NPROJ, 128), F32),
            pltpu.VMEM((PARTS, 2, 8, ROWS, 128), F32),
            pltpu.VMEM((PARTS, 8, ROWS, 128), F32),
            pltpu.VMEM((PARTS, 2, ROWS, 128), F32),
            pltpu.VMEM((PARTS, 2, 2, ROWS, 128), F32),
            pltpu.VMEM((PARTS, ROWS, 128), F32),
            pltpu.VMEM((PARTS, 2, ROWS, 128), F32),
            pltpu.VMEM((PARTS, ROWS, 128), F32),
            pltpu.VMEM((2, OWN, NB), BF16),
            pltpu.VMEM((2, OWN, NB), BF16),
            pltpu.VMEM((2, EXTRA, NB), BF16),
            pltpu.VMEM((2, EXTRA, NB), BF16),
            pltpu.VMEM((2 * NB, 2 * (OWN + EXTRA)), BF16),
            pltpu.VMEM((128, 128), F32),
            pltpu.VMEM((NB, COLS), F32),
            pltpu.VMEM((SLOTS, 16), jnp.int32),
            pltpu.SMEM((SLOTS, 16), jnp.int32),
            pltpu.VMEM((SLOTS, SLOTS), F32),
            pltpu.VMEM((2, SLOTS, 128), F32),
            pltpu.VMEM((NB, 2 * SLOTS), F32),
            pltpu.VMEM((2 * SLOTS, 2 * NB), F32),
            pltpu.VMEM((2, 2 * NB, NB), F32),
            pltpu.VMEM((NB, 2 * NB), F32),
            pltpu.VMEM((2, 2, 8, 2, 16, NB), F32),
            pltpu.VMEM((2, 8, 2, 16, NB), F32),
            pltpu.VMEM((2, 8, 2, 16, NB), F32),
            pltpu.VMEM((128, NPW), BF16),
            dma, dma((STEPS,)), dma,
            dma((PARTS,)), dma((PARTS,)),
            dma((PARTS, SUB, 6)), dma((PARTS, SUB, 2)), dma((PARTS, SUB, 2, 2)),
            dma((PARTS, SUB)), dma((PARTS, SUB)), dma((PARTS, SUB, 2)), dma((PARTS, SUB, 2)),
            dma((WCH,)), dma((WCH,)), dma((WCH,)), dma((WCH,)), dma((XCH,)), dma((XCH,)),
            dma((2,)), dma((2,)), dma((2, 8)), dma((2, 8)),
        ],
        compiler_params=pltpu.CompilerParams(collective_id=0, has_side_effects=True, vmem_limit_bytes=64 * 1024 * 1024 - 65536),
    )(
        projector_order.reshape(NPROJ // 128, 128),
        shift_map.reshape(NPW // 128, 128),
        atom_phase.reshape(1, 128),
        jnp.transpose(charges, (1, 2, 0)),
        waves,
        projectors,
    )
    return rows.reshape(1, 16, PARTS, 2, HALF).transpose(0, 1, 3, 2, 4).reshape(1, 16, 2, NB)


def solution(mesh):
    in_specs = (P("ka", None, "pw", None), P("ka", None, "pw", None), P(), P("pw"), P(), P())
    out_specs = P("ka", "pw", None, None)
    return jax.shard_map(local, mesh=mesh, in_specs=in_specs, out_specs=out_specs, check_vma=False)
```

```python
import jax
import jax.numpy as jnp
from jax import lax
from jax.experimental import pallas as pl
from jax.experimental.pallas import tpu as pltpu
from jax.sharding import PartitionSpec as P

MESH = pl.DeviceIdType.MESH
HIGH = lax.Precision.HIGHEST
F32 = jnp.float32
BF16 = jnp.bfloat16

NPW = 2048
NB = 256
PPA = 18
NPROJ = 2304
COLS = 768
STEPS = NPROJ // COLS
PARTS = 2
HALF = NB // PARTS
SLOTS = 144
SUB = 1
ROWS = 2 * SLOTS
OWN = NPW // 2
WCH = 8
WROWS = OWN // WCH
XCH = 4
EXTRA = OWN // 2
SPLIT = 2


def dot(a, b, dims=((1,), (0,)), precision=None):
    return lax.dot_general(a, b, (dims, ((), ())), precision=precision, preferred_element_type=F32)


def iota(shape, dim):
    return lax.broadcasted_iota(jnp.int32, shape, dim)


def kernel(
    order_ref, shift_ref, phase_ref, charges_ref, waves_ref, proj_ref, out_ref,
    wv, lt, beta, pu, ps, crecv, far, near, ydst, nxt, pk, xw, yw, ew, es, lp,
    colb, acc, invv, invs, sym, turn, bra, ket, plane, stage, oc, ocore, orecv, onehot,
    load_sem, beta_sem, inv_sem, core_s, core_r, x_s, far_r, near_r, y_s, y_r, n_s, n_r,
    w_s, w_r, f_s, f_r, e_s, e_r, oc_s, oc_r, o_s, o_r,
):
    me = lax.axis_index("pw")
    ka = lax.axis_index("ka")
    core = lax.rem(me, 2)
    j = me // 2
    x = lax.rem(j, 4)
    h = j // 4
    oh = 1 - h
    right = lax.rem(x + 1, 4)
    left = lax.rem(x + 3, 4)
    across = lax.rem(x + 2, 4)
    before = lax.rem(ka + 7, 8)
    after = lax.rem(ka + 1, 8)
    first = ka == 0
    last = ka == 7
    odd = lax.rem(ka, 2)
    partner = ka + 1 - 2 * odd
    beyond = lax.rem(ka + 2 + 4 * odd, 8)
    sent = OWN * (1 - odd)
    kept = OWN * odd

    def pw_of(hh, xx, cc):
        return (hh * 4 + xx) * 2 + cc

    def send(src, dst, s, r, pw, k):
        return pltpu.make_async_remote_copy(src_ref=src, dst_ref=dst, send_sem=s, recv_sem=r, device_id=(pw, k), device_id_type=MESH)

    load = pltpu.make_async_copy(waves_ref.at[0], wv, load_sem)
    load.start()

    def beta_copy(i):
        src = proj_ref.at[0, :, :, pl.ds(pl.multiple_of(i * COLS, COLS), COLS)]
        return pltpu.make_async_copy(src, beta.at[i], beta_sem.at[i])

    for i in range(2):
        beta_copy(i).start()

    pw_y = pw_of(oh, x, core)
    barrier = pltpu.get_barrier_semaphore()
    peers = [(lax.rem(me + d, 16), ka) for d in range(1, 16)]
    peers += [(me, lax.rem(ka + d, 8)) for d in (1, 2, 6, 7)]
    peers += [(pw_y, k) for k in (before, after)]
    for peer in peers:
        pl.semaphore_signal(barrier, inc=1, device_id=peer, device_id_type=MESH)

    order = jnp.concatenate([order_ref[pl.ds(r, 1), :] for r in range(NPROJ // 128)], axis=1)
    column = iota((SLOTS, NPROJ), 1)
    match_hi = (order >> 4) == iota((SLOTS, NPROJ), 0)
    match_lo = jnp.where((order & 15) == iota((16, NPROJ), 0), 1.0, 0.0).astype(BF16)
    digit_hi = jnp.where(match_hi, (column >> 7).astype(F32), 0.0).astype(BF16)
    digit_lo = jnp.where(match_hi, (column & 127).astype(F32), 0.0).astype(BF16)
    found = dot(digit_hi, match_lo, ((1,), (1,))) * 128.0 + dot(digit_lo, match_lo, ((1,), (1,)))
    invv[...] = jnp.clip(2 * found.astype(jnp.int32), 0, 2 * (NPROJ - 1))
    inv_copy = pltpu.make_async_copy(invv, invs, inv_sem)
    inv_copy.start()

    pl.semaphore_wait(barrier, len(peers))

    def piece(ref, c):
        return ref.at[:, pl.ds(c * WROWS, WROWS), :]

    def w_copy(c):
        src = waves_ref.at[0, :, pl.ds(pl.multiple_of(sent + c * WROWS, WROWS), WROWS), :]
        return send(src, piece(xw, c), w_s.at[c], w_r.at[c], me, partner)

    def f_copy(c):
        return send(piece(xw, c), piece(yw, c), f_s.at[c], f_r.at[c], me, beyond)

    def to_last(c):
        return send(piece(es, c), piece(yw, c), e_s.at[c], f_r.at[c], me, before)

    def to_first(c):
        src = waves_ref.at[0, :, pl.ds(OWN + EXTRA + c * WROWS, WROWS), :]
        return send(src, piece(ew, c), e_s.at[c], e_r.at[c], me, after)

    for c in range(WCH):
        w_copy(c).start()

    @pl.when(last)
    def _():
        for c in range(XCH):
            to_first(c).start()

    load.wait()
    for i in range(2, STEPS):
        beta_copy(i).start()

    for c in range(8):
        g = slice(256 * c, 256 * (c + 1))
        gi = slice(NPW + 256 * c, NPW + 256 * (c + 1))
        re = wv[0, g, :].T
        im = wv[1, g, :].T
        for p in range(PARTS):
            bands = slice(HALF * p, HALF * (p + 1))
            lt[NB * p : NB * p + HALF, g] = re[bands]
            lt[NB * p : NB * p + HALF, gi] = im[bands]
            lt[NB * p + HALF : NB * (p + 1), g] = im[bands]
            lt[NB * p + HALF : NB * (p + 1), gi] = -re[bands]

    def forward(lo, hi):
        for c in range(lo, hi):
            w_copy(c).wait_recv()

        @pl.when(ka != 1)
        def _():
            for c in range(lo, hi):
                f_copy(c).start()

    def choose(group):
        row = shift_ref[pl.ds(group, 1), :] - me * NPW
        want = jnp.broadcast_to(row.astype(F32), (128, 128)).T
        for t in range(NPW // 128):
            have = (iota((128, 128), 1) + 128 * t).astype(F32)
            onehot[:, 128 * t : 128 * (t + 1)] = jnp.where(want == have, 1.0, 0.0).astype(BF16)

    def extra_first():
        @pl.when(first)
        def _():
            def body(t, _):
                choose(OWN // 128 + t)
                for r in range(2):
                    es[r, pl.ds(pl.multiple_of(128 * t, 128), 128), :] = dot(onehot[...], wv[r]).astype(BF16)
                return 0

            lax.fori_loop(0, EXTRA // 128, body, 0)
            for c in range(XCH):
                to_last(c).start()

    def permute_first():
        @pl.when(first)
        def _():
            def body(t, _):
                choose(t + jnp.where(t >= OWN // 128, EXTRA // 128, 0))
                got = dot(lt[:, 0:NPW], onehot[...], ((1,), (1,))).astype(BF16)
                at = pl.multiple_of(128 * t, 128)
                lp[:, pl.ds(at, 128)] = got
                for p in range(PARTS):
                    lo = NB * p
                    lp[lo : lo + HALF, pl.ds(OWN + EXTRA + at, 128)] = got[lo + HALF : lo + NB]
                    lp[lo + HALF : lo + NB, pl.ds(OWN + EXTRA + at, 128)] = -got[lo : lo + HALF]
                return 0

            lax.fori_loop(0, (OWN + EXTRA) // 128, body, 0)

    def put(c, i):
        for q in range(2):
            pu[c, pl.ds(pl.multiple_of(2 * COLS * i, 8) + q, COLS, stride=2), :] = acc[HALF * q : HALF * (q + 1), :].T

    def project(c, lo, hi):
        def body(i, _):
            if c == 0:
                beta_copy(i).wait()
            put(c, jnp.maximum(i - 1, lo))
            acc[...] = dot(lt[NB * c : NB * (c + 1), :], beta[i].reshape(2 * NPW, COLS))
            return 0

        lax.fori_loop(lo, hi, body, 0)
        put(c, hi - 1)

    def gather(c, cr):
        def block(b, _):
            dst = ps.at[c, cr, b]

            def body(i, _):
                rows = [invs[9 * (2 * b + cr) + i, u] for u in range(16)]
                got = [pu[c, pl.ds(r, 2), :] for r in rows]
                for u in range(16):
                    dst[pl.ds(pl.multiple_of(32 * i, 32) + 2 * u, 2), :] = got[u]
                return 0

            return lax.fori_loop(0, SLOTS // 16, body, 0)

        lax.fori_loop(0, 8, block, 0)

    pw_core = pw_of(h, x, 1 - core)
    pw_right = pw_of(h, right, core)
    pw_left = pw_of(h, left, core)
    def core_copy(c):
        return send(ps.at[c, 1 - core], crecv.at[c], core_s.at[c], core_r.at[c], pw_core, ka)

    def spread_out(c):
        gather(c, 1 - core)
        core_copy(c).start()
        gather(c, core)

    def block_of(hh, xx):
        return hh * 4 + xx

    def sub(ref, e):
        return ref.at[pl.ds(e * (ROWS // SUB), ROWS // SUB), :]

    def mine(c, e, b):
        return sub(ps.at[c, core, b], e)

    def far_copy(c, e, d):
        return send(
            mine(c, e, block_of(d, across)), sub(far.at[c, d], e), x_s.at[c, e, d], far_r.at[c, e, d], (pw_right, pw_left)[d], ka
        )

    def near_copy(c, e, d, hh):
        return send(
            mine(c, e, block_of(hh, (right, left)[d])), sub(near.at[c, d, hh], e), x_s.at[c, e, 2 + 2 * d + hh],
            near_r.at[c, e, d, hh], (pw_right, pw_left)[d], ka,
        )

    def add_core(c, b):
        ps[c, core, b] += crecv[c, b]

    def ring_start(c):
        core_copy(c).wait_recv()
        for d in range(2):
            add_core(c, block_of(d, across))
            for e in range(SUB):
                far_copy(c, e, d).start()
        for d in range(2):
            add_core(c, block_of(1 - d, (right, left)[d]))
            for e in range(SUB):
                near_copy(c, e, d, 1 - d).start()
        for d in range(2):
            add_core(c, block_of(d, (right, left)[d]))
        for hh in range(2):
            add_core(c, block_of(hh, x))

    def add(c, e, b, ref):
        at = pl.ds(e * (ROWS // SUB), ROWS // SUB)
        total = ps[c, core, b, at, :]
        for one in ref:
            total += one[at, :]
        ps[c, core, b, at, :] = total

    def ring_rest(c):
        for e in range(SUB):
            for d in range(2):
                far_copy(c, e, d).wait_recv()
                add(c, e, block_of(d, (right, left)[d]), [far.at[c, d]])
                near_copy(c, e, d, d).start()

    def y_copy(c, e):
        return send(mine(c, e, block_of(oh, x)), sub(ydst.at[c], e), y_s.at[c, e], y_r.at[c, e], pw_y, ka)

    def n_copy(c, e, d):
        return send(
            mine(c, e, block_of((h, oh)[d], x)), sub(nxt.at[c, d], e), n_s.at[c, e, d], n_r.at[c, e, d], (me, pw_y)[d], before
        )

    def ring_end(c):
        for e in range(SUB):
            for d in range(2):
                for hh in range(2):
                    near_copy(c, e, d, hh).wait_recv()
            add(c, e, block_of(oh, x), [near.at[c, 0, oh], near.at[c, 1, oh]])
            y_copy(c, e).start()
            n_copy(c, e, 1).start()
            add(c, e, block_of(h, x), [near.at[c, 0, h], near.at[c, 1, h]])
            n_copy(c, e, 0).start()

    acc[...] = jnp.zeros_like(acc)
    project(0, 0, STEPS)
    inv_copy.wait()
    forward(0, 2)
    spread_out(0)
    forward(2, 4)
    project(1, 0, SPLIT)
    ring_start(0)
    project(1, SPLIT, STEPS)
    forward(4, 6)
    spread_out(1)
    extra_first()
    ring_rest(0)
    forward(6, 8)
    ring_start(1)

    atom_row = ((iota((SLOTS, SLOTS), 0).astype(F32) + 0.5) * (1.0 / PPA)).astype(jnp.int32)
    atom_col = ((iota((SLOTS, SLOTS), 1).astype(F32) + 0.5) * (1.0 / PPA)).astype(jnp.int32)
    spread = jnp.zeros((PPA, SLOTS), F32)
    for a in range(SLOTS // PPA):
        spread += jnp.where(iota((PPA, SLOTS), 1) == iota((PPA, SLOTS), 0) + PPA * a, 1.0, 0.0)
    slot = iota((SLOTS, 128), 0)
    atom = iota((SLOTS, 128), 1) - 8 * me
    flat = jnp.zeros((SLOTS, PPA), F32)
    for p in range(PPA):
        pick = jnp.where(slot == PPA * atom + p, 1.0, 0.0)
        flat += dot(pick, 0.5 * (charges_ref[p] + charges_ref[:, p, :]), ((1,), (1,)), HIGH)
    sym[...] = jnp.where(atom_row == atom_col, dot(flat, spread, precision=HIGH), 0.0)

    colb[...] = jnp.broadcast_to(phase_ref[...], (128, 128)).T
    own = colb[pl.ds(pl.multiple_of(8 * me, 8), 8), :]
    repeat = jnp.where(((iota((SLOTS, 8), 0).astype(F32) + 0.5) * (1.0 / PPA)).astype(jnp.int32) == iota((SLOTS, 8), 1), 1.0, 0.0)
    turn[0] = jnp.where(last, dot(repeat, jnp.cos(own), precision=HIGH), 1.0)
    turn[1] = jnp.where(last, dot(repeat, jnp.sin(own), precision=HIGH), 0.0)

    permute_first()
    ring_end(0)

    def product(left, at, width, parts):
        total = None
        for r in range(2):
            for ref, lo, n in parts:
                term = dot(left[:, pl.ds(pl.multiple_of(at + r * width + lo, 128), n)], ref[r, 0:n, :])
                total = term if total is None else total + term
        return total

    def f_wait(lo, hi):
        for c in range(lo, hi):
            f_copy(c).wait_recv()

    plane[odd] = product(lt, kept, NPW, [(xw, 0, OWN)])
    ring_rest(1)
    ring_end(1)

    @pl.when(jnp.logical_not(first | last))
    def _():
        f_wait(0, WCH)
        plane[1 - odd] = product(lt, kept, NPW, [(yw, 0, OWN)])

    @pl.when(last)
    def _():
        f_wait(0, XCH)
        plane[1 - odd] = product(lt, kept, NPW, [(yw, 0, EXTRA)])

    @pl.when(first)
    def _():
        f_wait(0, WCH)
        for c in range(XCH):
            to_first(c).wait_recv()
        plane[1 - odd] = product(lp, 0, OWN + EXTRA, [(yw, 0, OWN), (ew, OWN, EXTRA)])

    for c in range(PARTS):
        for r in range(2):
            lo = NB * c + HALF * r
            turned = plane[1, lo : lo + HALF, :].T
            for p in range(16):
                oc[1, p % 2, 2 * (p // 2 % 4) + p // 8, r, :, HALF * c : HALF * (c + 1)] = turned[16 * p : 16 * (p + 1)]

    def o_core(t):
        return send(oc.at[t, 1 - core], ocore.at[t], oc_s.at[t], oc_r.at[t], pw_core, ka)

    def o_copy(d):
        to = lax.rem(j + d, 8)
        return send(oc.at[0, core, to], orecv.at[0, d], o_s.at[0, d], o_r.at[0, d], 2 * to + core, ka)

    def o_add(t):
        o_core(t).wait_recv()
        for b in range(8):
            oc[t, core, b] += ocore[t, b]

    def p_copy(d):
        to = lax.rem(x + d, 4)
        at = pl.ds(2 * (d - 1), 2)
        return send(oc.at[1, core, pl.ds(2 * to, 2)], orecv.at[1, at], o_s.at[1, d], o_r.at[1, d], pw_of(h, to, core), ka)

    def q_copy(d):
        return send(oc.at[1, core, 2 * x + (h, oh)[d]], orecv.at[1, 6 + d], o_s.at[1, 4 + d], o_r.at[1, 4 + d], (me, pw_y)[d], before)

    o_core(1).start()

    def rows(ref, q):
        return ref[pl.ds(q, SLOTS, stride=2), :]

    def weigh(c):
        for e in range(SUB):
            for d in range(2):
                n_copy(c, e, d).wait_recv()
        nxt[c, 0] += nxt[c, 1]
        nr = rows(nxt.at[c, 0], 0)
        ni = rows(nxt.at[c, 0], 1)
        both = jnp.concatenate([nr * turn[0] + ni * turn[1], ni * turn[0] - nr * turn[1]], axis=1)
        weighted = dot(sym[...], both, precision=HIGH)
        wr = weighted[:, :HALF]
        wi = weighted[:, HALF:]
        ket[0:SLOTS, NB * c : NB * c + HALF] = wr
        ket[0:SLOTS, NB * c + HALF : NB * (c + 1)] = wi
        ket[SLOTS:, NB * c : NB * c + HALF] = wi
        ket[SLOTS:, NB * c + HALF : NB * (c + 1)] = -wr

    def hold(c):
        for e in range(SUB):
            y_copy(c, e).wait_recv()
        pk[c] = ps[c, core, block_of(h, x)] + ydst[c]
        for q in range(2):
            bra[HALF * c : HALF * (c + 1), SLOTS * q : SLOTS * (q + 1)] = rows(pk.at[c], q).T

    hold(0)
    weigh(0)
    o_add(1)
    for d in range(1, 4):
        p_copy(d).start()
    hold(1)
    weigh(1)
    stage[...] = dot(bra[...], ket[...], precision=HIGH)

    for p in range(16):
        at = slice(16 * p, 16 * (p + 1))
        lo = NB * (p // 8) + 16 * (p % 8)
        for c in range(PARTS):
            bands = slice(HALF * c, HALF * (c + 1))
            oc[0, p % 2, p // 2, 0, :, bands] = stage[at, NB * c : NB * c + HALF] + plane[0, lo : lo + 16, bands]
            oc[0, p % 2, p // 2, 1, :, bands] = stage[at, NB * c + HALF : NB * (c + 1)] - plane[0, lo + HALF : lo + HALF + 16, bands]
    o_core(0).start()

    for d in range(1, 4):
        p_copy(d).wait_recv()
        for hh in range(2):
            oc[1, core, 2 * x + hh] += orecv[1, 2 * (d - 1) + hh]
    for d in range(2):
        q_copy(d).start()
    o_add(0)
    for d in range(1, 8):
        o_copy(d).start()
    result = oc[0, core, j]
    for d in range(2):
        q_copy(d).wait_recv()
        result += orecv[1, 6 + d]
    for d in range(1, 8):
        o_copy(d).wait_recv()
        result += orecv[0, d]
    for r in range(2):
        for p in range(PARTS):
            out_ref[pl.ds(2 * p + r, 16, stride=4), :] = result[r][:, HALF * p : HALF * (p + 1)]

    for t in range(2):
        o_core(t).wait_send()
        q_copy(t).wait_send()
    for d in range(1, 8):
        o_copy(d).wait_send()
    for d in range(1, 4):
        p_copy(d).wait_send()
    for c in range(WCH):
        w_copy(c).wait_send()

    @pl.when(ka != 1)
    def _():
        for c in range(WCH):
            f_copy(c).wait_send()

    @pl.when(first)
    def _():
        for c in range(XCH):
            to_last(c).wait_send()

    @pl.when(last)
    def _():
        for c in range(XCH):
            to_first(c).wait_send()

    for c in range(PARTS):
        core_copy(c).wait_send()
        for e in range(SUB):
            y_copy(c, e).wait_send()
            for d in range(2):
                n_copy(c, e, d).wait_send()
                far_copy(c, e, d).wait_send()
                for hh in range(2):
                    near_copy(c, e, d, hh).wait_send()


def local(waves, projectors, projector_order, shift_map, charges, atom_phase):
    vmem = pl.BlockSpec(memory_space=pltpu.VMEM)
    hbm = pl.BlockSpec(memory_space=pl.ANY)
    dma = pltpu.SemaphoreType.DMA
    rows = pl.pallas_call(
        kernel,
        out_shape=jax.ShapeDtypeStruct((64, HALF), F32),
        in_specs=[vmem, vmem, vmem, vmem, hbm, hbm],
        out_specs=vmem,
        scratch_shapes=[
            pltpu.VMEM((2, NPW, NB), BF16),
            pltpu.VMEM((2 * NB, 2 * NPW), BF16),
            pltpu.VMEM((STEPS, 2, NPW, COLS), BF16),
            pltpu.VMEM((PARTS, 2 * NPROJ, 128), F32),
            pltpu.VMEM((PARTS, 2, 8, ROWS, 128), F32),
            pltpu.VMEM((PARTS, 8, ROWS, 128), F32),
            pltpu.VMEM((PARTS, 2, ROWS, 128), F32),
            pltpu.VMEM((PARTS, 2, 2, ROWS, 128), F32),
            pltpu.VMEM((PARTS, ROWS, 128), F32),
            pltpu.VMEM((PARTS, 2, ROWS, 128), F32),
            pltpu.VMEM((PARTS, ROWS, 128), F32),
            pltpu.VMEM((2, OWN, NB), BF16),
            pltpu.VMEM((2, OWN, NB), BF16),
            pltpu.VMEM((2, EXTRA, NB), BF16),
            pltpu.VMEM((2, EXTRA, NB), BF16),
            pltpu.VMEM((2 * NB, 2 * (OWN + EXTRA)), BF16),
            pltpu.VMEM((128, 128), F32),
            pltpu.VMEM((NB, COLS), F32),
            pltpu.VMEM((SLOTS, 16), jnp.int32),
            pltpu.SMEM((SLOTS, 16), jnp.int32),
            pltpu.VMEM((SLOTS, SLOTS), F32),
            pltpu.VMEM((2, SLOTS, 128), F32),
            pltpu.VMEM((NB, 2 * SLOTS), F32),
            pltpu.VMEM((2 * SLOTS, 2 * NB), F32),
            pltpu.VMEM((2, 2 * NB, NB), F32),
            pltpu.VMEM((NB, 2 * NB), F32),
            pltpu.VMEM((2, 2, 8, 2, 16, NB), F32),
            pltpu.VMEM((2, 8, 2, 16, NB), F32),
            pltpu.VMEM((2, 8, 2, 16, NB), F32),
            pltpu.VMEM((128, NPW), BF16),
            dma, dma((STEPS,)), dma,
            dma((PARTS,)), dma((PARTS,)),
            dma((PARTS, SUB, 6)), dma((PARTS, SUB, 2)), dma((PARTS, SUB, 2, 2)),
            dma((PARTS, SUB)), dma((PARTS, SUB)), dma((PARTS, SUB, 2)), dma((PARTS, SUB, 2)),
            dma((WCH,)), dma((WCH,)), dma((WCH,)), dma((WCH,)), dma((XCH,)), dma((XCH,)),
            dma((2,)), dma((2,)), dma((2, 8)), dma((2, 8)),
        ],
        compiler_params=pltpu.CompilerParams(collective_id=0, has_side_effects=True, vmem_limit_bytes=64 * 1024 * 1024 - 65536),
    )(
        projector_order.reshape(NPROJ // 128, 128),
        shift_map.reshape(NPW // 128, 128),
        atom_phase.reshape(1, 128),
        jnp.transpose(charges, (1, 2, 0)),
        waves,
        projectors,
    )
    return rows.reshape(1, 16, PARTS, 2, HALF).transpose(0, 1, 3, 2, 4).reshape(1, 16, 2, NB)


def solution(mesh):
    in_specs = (P("ka", None, "pw", None), P("ka", None, "pw", None), P(), P("pw"), P(), P())
    out_specs = P("ka", "pw", None, None)
    return jax.shard_map(local, mesh=mesh, in_specs=in_specs, out_specs=out_specs, check_vma=False)
```

```python
import jax
import jax.numpy as jnp
from jax import lax
from jax.experimental import pallas as pl
from jax.experimental.pallas import tpu as pltpu
from jax.sharding import PartitionSpec as P

MESH = pl.DeviceIdType.MESH
HIGH = lax.Precision.HIGHEST
F32 = jnp.float32
BF16 = jnp.bfloat16

NPW = 2048
NB = 256
PPA = 18
NPROJ = 2304
COLS = 768
STEPS = NPROJ // COLS
PARTS = 2
HALF = NB // PARTS
SLOTS = 144
SUB = 1
ROWS = 2 * SLOTS
OWN = NPW // 2
WCH = 8
WROWS = OWN // WCH
XCH = 4
EXTRA = OWN // 2
SPLIT = 2


def dot(a, b, dims=((1,), (0,)), precision=None):
    return lax.dot_general(a, b, (dims, ((), ())), precision=precision, preferred_element_type=F32)


def iota(shape, dim):
    return lax.broadcasted_iota(jnp.int32, shape, dim)


def kernel(
    order_ref, shift_ref, phase_ref, charges_ref, waves_ref, proj_ref, out_ref,
    wv, lt, beta, pu, ps, crecv, far, near, ydst, nxt, pk, xw, yw, ew, es, lp,
    colb, acc, invv, invs, sym, turn, bra, ket, plane, stage, oc, ocore, orecv, onehot,
    load_sem, beta_sem, inv_sem, core_s, core_r, x_s, far_r, near_r, y_s, y_r, n_s, n_r,
    w_s, w_r, f_s, f_r, e_s, e_r, oc_s, oc_r, o_s, o_r,
):
    me = lax.axis_index("pw")
    ka = lax.axis_index("ka")
    core = lax.rem(me, 2)
    j = me // 2
    x = lax.rem(j, 4)
    h = j // 4
    oh = 1 - h
    right = lax.rem(x + 1, 4)
    left = lax.rem(x + 3, 4)
    across = lax.rem(x + 2, 4)
    before = lax.rem(ka + 7, 8)
    after = lax.rem(ka + 1, 8)
    first = ka == 0
    last = ka == 7
    odd = lax.rem(ka, 2)
    partner = ka + 1 - 2 * odd
    beyond = lax.rem(ka + 2 + 4 * odd, 8)
    sent = OWN * (1 - odd)
    kept = OWN * odd

    def pw_of(hh, xx, cc):
        return (hh * 4 + xx) * 2 + cc

    def send(src, dst, s, r, pw, k):
        return pltpu.make_async_remote_copy(src_ref=src, dst_ref=dst, send_sem=s, recv_sem=r, device_id=(pw, k), device_id_type=MESH)

    load = pltpu.make_async_copy(waves_ref.at[0], wv, load_sem)
    load.start()

    def beta_copy(i):
        src = proj_ref.at[0, :, :, pl.ds(pl.multiple_of(i * COLS, COLS), COLS)]
        return pltpu.make_async_copy(src, beta.at[i], beta_sem.at[i])

    for i in range(2):
        beta_copy(i).start()

    pw_y = pw_of(oh, x, core)
    barrier = pltpu.get_barrier_semaphore()
    peers = [(lax.rem(me + d, 16), ka) for d in range(1, 16)]
    peers += [(me, lax.rem(ka + d, 8)) for d in (1, 2, 6, 7)]
    peers += [(pw_y, k) for k in (before, after)]
    for peer in peers:
        pl.semaphore_signal(barrier, inc=1, device_id=peer, device_id_type=MESH)

    order = jnp.concatenate([order_ref[pl.ds(r, 1), :] for r in range(NPROJ // 128)], axis=1)
    column = iota((SLOTS, NPROJ), 1)
    match_hi = (order >> 4) == iota((SLOTS, NPROJ), 0)
    match_lo = jnp.where((order & 15) == iota((16, NPROJ), 0), 1.0, 0.0).astype(BF16)
    digit_hi = jnp.where(match_hi, (column >> 7).astype(F32), 0.0).astype(BF16)
    digit_lo = jnp.where(match_hi, (column & 127).astype(F32), 0.0).astype(BF16)
    found = dot(digit_hi, match_lo, ((1,), (1,))) * 128.0 + dot(digit_lo, match_lo, ((1,), (1,)))
    invv[...] = jnp.clip(2 * found.astype(jnp.int32), 0, 2 * (NPROJ - 1))
    inv_copy = pltpu.make_async_copy(invv, invs, inv_sem)
    inv_copy.start()

    pl.semaphore_wait(barrier, len(peers))

    def piece(ref, c):
        return ref.at[:, pl.ds(c * WROWS, WROWS), :]

    def w_copy(c):
        src = waves_ref.at[0, :, pl.ds(pl.multiple_of(sent + c * WROWS, WROWS), WROWS), :]
        return send(src, piece(xw, c), w_s.at[c], w_r.at[c], me, partner)

    def f_copy(c):
        return send(piece(xw, c), piece(yw, c), f_s.at[c], f_r.at[c], me, beyond)

    def to_last(c):
        return send(piece(es, c), piece(yw, c), e_s.at[c], f_r.at[c], me, before)

    def to_first(c):
        src = waves_ref.at[0, :, pl.ds(OWN + EXTRA + c * WROWS, WROWS), :]
        return send(src, piece(ew, c), e_s.at[c], e_r.at[c], me, after)

    for c in range(WCH):
        w_copy(c).start()

    @pl.when(last)
    def _():
        for c in range(XCH):
            to_first(c).start()

    load.wait()
    for i in range(2, STEPS):
        beta_copy(i).start()

    for c in range(8):
        g = slice(256 * c, 256 * (c + 1))
        gi = slice(NPW + 256 * c, NPW + 256 * (c + 1))
        re = wv[0, g, :].T
        im = wv[1, g, :].T
        for p in range(PARTS):
            bands = slice(HALF * p, HALF * (p + 1))
            lt[NB * p : NB * p + HALF, g] = re[bands]
            lt[NB * p : NB * p + HALF, gi] = im[bands]
            lt[NB * p + HALF : NB * (p + 1), g] = im[bands]
            lt[NB * p + HALF : NB * (p + 1), gi] = -re[bands]

    def forward(lo, hi):
        for c in range(lo, hi):
            w_copy(c).wait_recv()

        @pl.when(ka != 1)
        def _():
            for c in range(lo, hi):
                f_copy(c).start()

    def choose(group):
        row = shift_ref[pl.ds(group, 1), :] - me * NPW
        want = jnp.broadcast_to(row.astype(F32), (128, 128)).T
        for t in range(NPW // 128):
            have = (iota((128, 128), 1) + 128 * t).astype(F32)
            onehot[:, 128 * t : 128 * (t + 1)] = jnp.where(want == have, 1.0, 0.0).astype(BF16)

    def extra_first():
        @pl.when(first)
        def _():
            def body(t, _):
                choose(OWN // 128 + t)
                for r in range(2):
                    es[r, pl.ds(pl.multiple_of(128 * t, 128), 128), :] = dot(onehot[...], wv[r]).astype(BF16)
                return 0

            lax.fori_loop(0, EXTRA // 128, body, 0)
            for c in range(XCH):
                to_last(c).start()

    def permute_first():
        @pl.when(first)
        def _():
            def body(t, _):
                choose(t + jnp.where(t >= OWN // 128, EXTRA // 128, 0))
                got = dot(lt[:, 0:NPW], onehot[...], ((1,), (1,))).astype(BF16)
                at = pl.multiple_of(128 * t, 128)
                lp[:, pl.ds(at, 128)] = got
                for p in range(PARTS):
                    lo = NB * p
                    lp[lo : lo + HALF, pl.ds(OWN + EXTRA + at, 128)] = got[lo + HALF : lo + NB]
                    lp[lo + HALF : lo + NB, pl.ds(OWN + EXTRA + at, 128)] = -got[lo : lo + HALF]
                return 0

            lax.fori_loop(0, (OWN + EXTRA) // 128, body, 0)

    def put(c, i):
        for q in range(2):
            pu[c, pl.ds(pl.multiple_of(2 * COLS * i, 8) + q, COLS, stride=2), :] = acc[HALF * q : HALF * (q + 1), :].T

    def project(c, lo, hi):
        def body(i, _):
            if c == 0:
                beta_copy(i).wait()
            put(c, jnp.maximum(i - 1, lo))
            acc[...] = dot(lt[NB * c : NB * (c + 1), :], beta[i].reshape(2 * NPW, COLS))
            return 0

        lax.fori_loop(lo, hi, body, 0)
        put(c, hi - 1)

    def gather(c, cr):
        def block(b, _):
            dst = ps.at[c, cr, b]

            def body(i, _):
                rows = [invs[9 * (2 * b + cr) + i, u] for u in range(16)]
                got = [pu[c, pl.ds(r, 2), :] for r in rows]
                for u in range(16):
                    dst[pl.ds(pl.multiple_of(32 * i, 32) + 2 * u, 2), :] = got[u]
                return 0

            return lax.fori_loop(0, SLOTS // 16, body, 0)

        lax.fori_loop(0, 8, block, 0)

    pw_core = pw_of(h, x, 1 - core)
    pw_right = pw_of(h, right, core)
    pw_left = pw_of(h, left, core)
    def core_copy(c):
        return send(ps.at[c, 1 - core], crecv.at[c], core_s.at[c], core_r.at[c], pw_core, ka)

    def spread_out(c):
        gather(c, 1 - core)
        core_copy(c).start()
        gather(c, core)

    def block_of(hh, xx):
        return hh * 4 + xx

    def sub(ref, e):
        return ref.at[pl.ds(e * (ROWS // SUB), ROWS // SUB), :]

    def mine(c, e, b):
        return sub(ps.at[c, core, b], e)

    def far_copy(c, e, d):
        return send(
            mine(c, e, block_of(d, across)), sub(far.at[c, d], e), x_s.at[c, e, d], far_r.at[c, e, d], (pw_right, pw_left)[d], ka
        )

    def near_copy(c, e, d, hh):
        return send(
            mine(c, e, block_of(hh, (right, left)[d])), sub(near.at[c, d, hh], e), x_s.at[c, e, 2 + 2 * d + hh],
            near_r.at[c, e, d, hh], (pw_right, pw_left)[d], ka,
        )

    def add_core(c, b):
        ps[c, core, b] += crecv[c, b]

    def ring_start(c):
        core_copy(c).wait_recv()
        for d in range(2):
            add_core(c, block_of(d, across))
            for e in range(SUB):
                far_copy(c, e, d).start()
        for d in range(2):
            add_core(c, block_of(1 - d, (right, left)[d]))
            for e in range(SUB):
                near_copy(c, e, d, 1 - d).start()
        for d in range(2):
            add_core(c, block_of(d, (right, left)[d]))
        for hh in range(2):
            add_core(c, block_of(hh, x))

    def add(c, e, b, ref):
        at = pl.ds(e * (ROWS // SUB), ROWS // SUB)
        total = ps[c, core, b, at, :]
        for one in ref:
            total += one[at, :]
        ps[c, core, b, at, :] = total

    def ring_rest(c):
        for e in range(SUB):
            for d in range(2):
                far_copy(c, e, d).wait_recv()
                add(c, e, block_of(d, (right, left)[d]), [far.at[c, d]])
                near_copy(c, e, d, d).start()

    def y_copy(c, e):
        return send(mine(c, e, block_of(oh, x)), sub(ydst.at[c], e), y_s.at[c, e], y_r.at[c, e], pw_y, ka)

    def n_copy(c, e, d):
        return send(
            mine(c, e, block_of((h, oh)[d], x)), sub(nxt.at[c, d], e), n_s.at[c, e, d], n_r.at[c, e, d], (me, pw_y)[d], before
        )

    def ring_end(c):
        for e in range(SUB):
            for d in range(2):
                for hh in range(2):
                    near_copy(c, e, d, hh).wait_recv()
            add(c, e, block_of(oh, x), [near.at[c, 0, oh], near.at[c, 1, oh]])
            y_copy(c, e).start()
            n_copy(c, e, 1).start()
            add(c, e, block_of(h, x), [near.at[c, 0, h], near.at[c, 1, h]])
            n_copy(c, e, 0).start()

    acc[...] = jnp.zeros_like(acc)
    project(0, 0, STEPS)
    inv_copy.wait()
    forward(0, 2)
    spread_out(0)
    forward(2, 4)
    project(1, 0, SPLIT)
    ring_start(0)
    project(1, SPLIT, STEPS)
    forward(4, 6)
    spread_out(1)
    extra_first()
    ring_rest(0)
    forward(6, 8)
    ring_start(1)

    atom_row = ((iota((SLOTS, SLOTS), 0).astype(F32) + 0.5) * (1.0 / PPA)).astype(jnp.int32)
    atom_col = ((iota((SLOTS, SLOTS), 1).astype(F32) + 0.5) * (1.0 / PPA)).astype(jnp.int32)
    spread = jnp.zeros((PPA, SLOTS), F32)
    for a in range(SLOTS // PPA):
        spread += jnp.where(iota((PPA, SLOTS), 1) == iota((PPA, SLOTS), 0) + PPA * a, 1.0, 0.0)
    slot = iota((SLOTS, 128), 0)
    atom = iota((SLOTS, 128), 1) - 8 * me
    flat = jnp.zeros((SLOTS, PPA), F32)
    for p in range(PPA):
        pick = jnp.where(slot == PPA * atom + p, 1.0, 0.0)
        flat += dot(pick, 0.5 * (charges_ref[p] + charges_ref[:, p, :]), ((1,), (1,)), HIGH)
    sym[...] = jnp.where(atom_row == atom_col, dot(flat, spread, precision=HIGH), 0.0)

    colb[...] = jnp.broadcast_to(phase_ref[...], (128, 128)).T
    own = colb[pl.ds(pl.multiple_of(8 * me, 8), 8), :]
    repeat = jnp.where(((iota((SLOTS, 8), 0).astype(F32) + 0.5) * (1.0 / PPA)).astype(jnp.int32) == iota((SLOTS, 8), 1), 1.0, 0.0)
    turn[0] = jnp.where(last, dot(repeat, jnp.cos(own), precision=HIGH), 1.0)
    turn[1] = jnp.where(last, dot(repeat, jnp.sin(own), precision=HIGH), 0.0)

    permute_first()
    ring_end(0)

    def product(left, at, width, parts):
        total = None
        for r in range(2):
            for ref, lo, n in parts:
                term = dot(left[:, pl.ds(pl.multiple_of(at + r * width + lo, 128), n)], ref[r, 0:n, :])
                total = term if total is None else total + term
        return total

    def f_wait(lo, hi):
        for c in range(lo, hi):
            f_copy(c).wait_recv()

    plane[odd] = product(lt, kept, NPW, [(xw, 0, OWN)])
    ring_rest(1)
    ring_end(1)

    @pl.when(jnp.logical_not(first | last))
    def _():
        f_wait(0, WCH)
        plane[1 - odd] = product(lt, kept, NPW, [(yw, 0, OWN)])

    @pl.when(last)
    def _():
        f_wait(0, XCH)
        plane[1 - odd] = product(lt, kept, NPW, [(yw, 0, EXTRA)])

    @pl.when(first)
    def _():
        f_wait(0, WCH)
        for c in range(XCH):
            to_first(c).wait_recv()
        plane[1 - odd] = product(lp, 0, OWN + EXTRA, [(yw, 0, OWN), (ew, OWN, EXTRA)])

    for c in range(PARTS):
        for r in range(2):
            lo = NB * c + HALF * r
            turned = plane[1, lo : lo + HALF, :].T
            for p in range(16):
                oc[1, p % 2, 2 * (p // 2 % 4) + p // 8, r, :, HALF * c : HALF * (c + 1)] = turned[16 * p : 16 * (p + 1)]

    def o_core(t):
        return send(oc.at[t, 1 - core], ocore.at[t], oc_s.at[t], oc_r.at[t], pw_core, ka)

    def o_copy(d):
        to = lax.rem(j + d, 8)
        return send(oc.at[0, core, to], orecv.at[0, d], o_s.at[0, d], o_r.at[0, d], 2 * to + core, ka)

    def o_add(t):
        o_core(t).wait_recv()
        for b in range(8):
            oc[t, core, b] += ocore[t, b]

    def p_copy(d):
        to = lax.rem(x + d, 4)
        at = pl.ds(2 * (d - 1), 2)
        return send(oc.at[1, core, pl.ds(2 * to, 2)], orecv.at[1, at], o_s.at[1, d], o_r.at[1, d], pw_of(h, to, core), ka)

    def q_copy(d):
        return send(oc.at[1, core, 2 * x + (h, oh)[d]], orecv.at[1, 6 + d], o_s.at[1, 4 + d], o_r.at[1, 4 + d], (me, pw_y)[d], before)

    o_core(1).start()

    def rows(ref, q):
        return ref[pl.ds(q, SLOTS, stride=2), :]

    def weigh(c):
        for e in range(SUB):
            for d in range(2):
                n_copy(c, e, d).wait_recv()
        nxt[c, 0] += nxt[c, 1]
        nr = rows(nxt.at[c, 0], 0)
        ni = rows(nxt.at[c, 0], 1)
        both = jnp.concatenate([nr * turn[0] + ni * turn[1], ni * turn[0] - nr * turn[1]], axis=1)
        weighted = dot(sym[...], both, precision=HIGH)
        wr = weighted[:, :HALF]
        wi = weighted[:, HALF:]
        ket[0:SLOTS, NB * c : NB * c + HALF] = wr
        ket[0:SLOTS, NB * c + HALF : NB * (c + 1)] = wi
        ket[SLOTS:, NB * c : NB * c + HALF] = wi
        ket[SLOTS:, NB * c + HALF : NB * (c + 1)] = -wr

    def hold(c):
        for e in range(SUB):
            y_copy(c, e).wait_recv()
        pk[c] = ps[c, core, block_of(h, x)] + ydst[c]
        for q in range(2):
            bra[HALF * c : HALF * (c + 1), SLOTS * q : SLOTS * (q + 1)] = rows(pk.at[c], q).T

    hold(0)
    weigh(0)
    o_add(1)
    for d in range(1, 4):
        p_copy(d).start()
    def margin(c):
        bands = slice(HALF * c, HALF * (c + 1))
        stage[:, NB * c : NB * (c + 1)] = dot(bra[...], ket[:, NB * c : NB * (c + 1)], precision=HIGH)
        for p in range(16):
            at = slice(16 * p, 16 * (p + 1))
            lo = NB * (p // 8) + 16 * (p % 8)
            oc[0, p % 2, p // 2, 0, :, bands] = stage[at, NB * c : NB * c + HALF] + plane[0, lo : lo + 16, bands]
            oc[0, p % 2, p // 2, 1, :, bands] = stage[at, NB * c + HALF : NB * (c + 1)] - plane[0, lo + HALF : lo + HALF + 16, bands]

    hold(1)
    margin(0)
    weigh(1)
    margin(1)
    o_core(0).start()

    for d in range(1, 4):
        p_copy(d).wait_recv()
        for hh in range(2):
            oc[1, core, 2 * x + hh] += orecv[1, 2 * (d - 1) + hh]
    for d in range(2):
        q_copy(d).start()
    o_add(0)
    for d in range(1, 8):
        o_copy(d).start()
    result = oc[0, core, j]
    for d in range(2):
        q_copy(d).wait_recv()
        result += orecv[1, 6 + d]
    for d in range(1, 8):
        o_copy(d).wait_recv()
        result += orecv[0, d]
    for r in range(2):
        for p in range(PARTS):
            out_ref[pl.ds(2 * p + r, 16, stride=4), :] = result[r][:, HALF * p : HALF * (p + 1)]

    for t in range(2):
        o_core(t).wait_send()
        q_copy(t).wait_send()
    for d in range(1, 8):
        o_copy(d).wait_send()
    for d in range(1, 4):
        p_copy(d).wait_send()
    for c in range(WCH):
        w_copy(c).wait_send()

    @pl.when(ka != 1)
    def _():
        for c in range(WCH):
            f_copy(c).wait_send()

    @pl.when(first)
    def _():
        for c in range(XCH):
            to_last(c).wait_send()

    @pl.when(last)
    def _():
        for c in range(XCH):
            to_first(c).wait_send()

    for c in range(PARTS):
        core_copy(c).wait_send()
        for e in range(SUB):
            y_copy(c, e).wait_send()
            for d in range(2):
                n_copy(c, e, d).wait_send()
                far_copy(c, e, d).wait_send()
                for hh in range(2):
                    near_copy(c, e, d, hh).wait_send()


def local(waves, projectors, projector_order, shift_map, charges, atom_phase):
    vmem = pl.BlockSpec(memory_space=pltpu.VMEM)
    hbm = pl.BlockSpec(memory_space=pl.ANY)
    dma = pltpu.SemaphoreType.DMA
    rows = pl.pallas_call(
        kernel,
        out_shape=jax.ShapeDtypeStruct((64, HALF), F32),
        in_specs=[vmem, vmem, vmem, vmem, hbm, hbm],
        out_specs=vmem,
        scratch_shapes=[
            pltpu.VMEM((2, NPW, NB), BF16),
            pltpu.VMEM((2 * NB, 2 * NPW), BF16),
            pltpu.VMEM((STEPS, 2, NPW, COLS), BF16),
            pltpu.VMEM((PARTS, 2 * NPROJ, 128), F32),
            pltpu.VMEM((PARTS, 2, 8, ROWS, 128), F32),
            pltpu.VMEM((PARTS, 8, ROWS, 128), F32),
            pltpu.VMEM((PARTS, 2, ROWS, 128), F32),
            pltpu.VMEM((PARTS, 2, 2, ROWS, 128), F32),
            pltpu.VMEM((PARTS, ROWS, 128), F32),
            pltpu.VMEM((PARTS, 2, ROWS, 128), F32),
            pltpu.VMEM((PARTS, ROWS, 128), F32),
            pltpu.VMEM((2, OWN, NB), BF16),
            pltpu.VMEM((2, OWN, NB), BF16),
            pltpu.VMEM((2, EXTRA, NB), BF16),
            pltpu.VMEM((2, EXTRA, NB), BF16),
            pltpu.VMEM((2 * NB, 2 * (OWN + EXTRA)), BF16),
            pltpu.VMEM((128, 128), F32),
            pltpu.VMEM((NB, COLS), F32),
            pltpu.VMEM((SLOTS, 16), jnp.int32),
            pltpu.SMEM((SLOTS, 16), jnp.int32),
            pltpu.VMEM((SLOTS, SLOTS), F32),
            pltpu.VMEM((2, SLOTS, 128), F32),
            pltpu.VMEM((NB, 2 * SLOTS), F32),
            pltpu.VMEM((2 * SLOTS, 2 * NB), F32),
            pltpu.VMEM((2, 2 * NB, NB), F32),
            pltpu.VMEM((NB, 2 * NB), F32),
            pltpu.VMEM((2, 2, 8, 2, 16, NB), F32),
            pltpu.VMEM((2, 8, 2, 16, NB), F32),
            pltpu.VMEM((2, 8, 2, 16, NB), F32),
            pltpu.VMEM((128, NPW), BF16),
            dma, dma((STEPS,)), dma,
            dma((PARTS,)), dma((PARTS,)),
            dma((PARTS, SUB, 6)), dma((PARTS, SUB, 2)), dma((PARTS, SUB, 2, 2)),
            dma((PARTS, SUB)), dma((PARTS, SUB)), dma((PARTS, SUB, 2)), dma((PARTS, SUB, 2)),
            dma((WCH,)), dma((WCH,)), dma((WCH,)), dma((WCH,)), dma((XCH,)), dma((XCH,)),
            dma((2,)), dma((2,)), dma((2, 8)), dma((2, 8)),
        ],
        compiler_params=pltpu.CompilerParams(collective_id=0, has_side_effects=True, vmem_limit_bytes=64 * 1024 * 1024 - 65536),
    )(
        projector_order.reshape(NPROJ // 128, 128),
        shift_map.reshape(NPW // 128, 128),
        atom_phase.reshape(1, 128),
        jnp.transpose(charges, (1, 2, 0)),
        waves,
        projectors,
    )
    return rows.reshape(1, 16, PARTS, 2, HALF).transpose(0, 1, 3, 2, 4).reshape(1, 16, 2, NB)


def solution(mesh):
    in_specs = (P("ka", None, "pw", None), P("ka", None, "pw", None), P(), P("pw"), P(), P())
    out_specs = P("ka", "pw", None, None)
    return jax.shard_map(local, mesh=mesh, in_specs=in_specs, out_specs=out_specs, check_vma=False)
```
